64 devices in a mesh: data: 4 (over x, y), seq: 16 (over z, core).
Axes of the slice: x: 2, y: 2, z: 8, core: 2. Of those that a mesh axis runs over, the one named last changes fastest.
The devices are a block of a 4x4x8 slice.
Arguments:
- patches: bfloat16 [256, 512, 512], P('data', 'seq'), parts along dimension 0
- ln1_gain: float32 [512], replicated
- ln1_bias: float32 [512], replicated
- w_in: bfloat16 [512, 3072], replicated
- b_in: float32 [3072], replicated
- ln2_gain: float32 [1536], replicated
- ln2_bias: float32 [1536], replicated
- w_spatial: bfloat16 [512, 512], replicated
- b_spatial: float32 [512], replicated
- w_out: bfloat16 [1536, 512], replicated
- b_out: float32 [512], replicated
Outputs:
- output: bfloat16 [256, 512, 512], P('data', 'seq'), parts along dimension 0
There are 4 independent parts. The reference program is written for one: setup_inputs(seed, part) draws one part's arguments, and reference() takes and returns one part's arrays. A program takes and returns all parts, laid end to end along the dimension named above; an argument that names none is the same for every part.
All inputs are finite; a program needn't handle non-finite values.
Results may differ from the reference program's by a relative error of at most 0.00927909.
Values are sent between devices in bfloat16 or wider.
A program may use at most 768 MiB of HBM per device.

```python
import jax
import jax.numpy as jnp
from jax import lax

BATCH_SIZE = 64
NUM_PATCHES = 512
MODEL_DIM = 512
GATE_DIM = 1536
LN_EPS = 1e-6


def layer_norm(values, gain_vec, offset):
    values_f = values.astype(jnp.float32)
    mean_val = jnp.mean(values_f, axis=-1, keepdims=True)
    centered = values_f - mean_val
    var_val = jnp.mean(centered * centered, axis=-1, keepdims=True)
    return (centered * lax.rsqrt(var_val + LN_EPS) * gain_vec + offset).astype(jnp.bfloat16)


def setup_inputs(seed: int = 0, part: int = 0) -> dict:
    key_list = jax.random.split(jax.random.key(seed), 11)
    part_key = jax.random.fold_in(key_list[0], part)
    two_gate = 2 * GATE_DIM
    patches = jax.random.normal(part_key, (BATCH_SIZE, NUM_PATCHES, MODEL_DIM), jnp.float32)
    ln1_gain = 1.0 + 0.3 * jax.random.normal(key_list[1], (MODEL_DIM,), jnp.float32)
    ln1_bias = 0.3 * jax.random.normal(key_list[2], (MODEL_DIM,), jnp.float32)
    w_in = jax.random.normal(key_list[3], (MODEL_DIM, two_gate), jnp.float32) * MODEL_DIM ** -0.5
    b_in = 0.3 * jax.random.normal(key_list[4], (two_gate,), jnp.float32)
    ln2_gain = 1.0 + 0.3 * jax.random.normal(key_list[5], (GATE_DIM,), jnp.float32)
    ln2_bias = 0.3 * jax.random.normal(key_list[6], (GATE_DIM,), jnp.float32)
    w_spatial = jax.random.normal(key_list[7], (NUM_PATCHES, NUM_PATCHES), jnp.float32) * NUM_PATCHES ** -0.5
    b_spatial = 1.0 + 0.5 * jax.random.normal(key_list[8], (NUM_PATCHES,), jnp.float32)
    w_out = jax.random.normal(key_list[9], (GATE_DIM, MODEL_DIM), jnp.float32) * GATE_DIM ** -0.5
    b_out = 0.3 * jax.random.normal(key_list[10], (MODEL_DIM,), jnp.float32)
    return {
        "patches": patches.astype(jnp.bfloat16),
        "ln1_gain": ln1_gain,
        "ln1_bias": ln1_bias,
        "w_in": w_in.astype(jnp.bfloat16),
        "b_in": b_in,
        "ln2_gain": ln2_gain,
        "ln2_bias": ln2_bias,
        "w_spatial": w_spatial.astype(jnp.bfloat16),
        "b_spatial": b_spatial,
        "w_out": w_out.astype(jnp.bfloat16),
        "b_out": b_out,
    }


def reference(patches, ln1_gain, ln1_bias, w_in, b_in, ln2_gain, ln2_bias, w_spatial, b_spatial, w_out, b_out):
    half_dim = w_out.shape[0]

    def one_image(image):
        normed = layer_norm(image, ln1_gain, ln1_bias)
        hidden = jnp.dot(normed, w_in, preferred_element_type=jnp.float32) + b_in
        hidden = jax.nn.gelu(hidden, approximate=False).astype(jnp.bfloat16)
        gate_a = hidden[:, :half_dim]
        gate_n = layer_norm(hidden[:, half_dim:], ln2_gain, ln2_bias)
        spatial = jnp.dot(w_spatial.T, gate_n, preferred_element_type=jnp.float32).astype(jnp.bfloat16)
        gated = (gate_a.astype(jnp.float32) * (spatial.astype(jnp.float32) + b_spatial[:, None])).astype(jnp.bfloat16)
        mixed = jnp.dot(gated, w_out, preferred_element_type=jnp.float32) + b_out
        return (image.astype(jnp.float32) + mixed).astype(jnp.bfloat16)

    return lax.map(one_image, patches)
```

```python
import jax
import jax.numpy as jnp
from jax import lax
from jax.sharding import PartitionSpec as P

LN_EPS = 1e-6


def layer_norm(values, gain_vec, offset):
    values_f = values.astype(jnp.float32)
    mean_val = jnp.mean(values_f, axis=-1, keepdims=True)
    centered = values_f - mean_val
    var_val = jnp.mean(centered * centered, axis=-1, keepdims=True)
    return (centered * lax.rsqrt(var_val + LN_EPS) * gain_vec + offset).astype(jnp.bfloat16)


def gelu_proj(normed, weight, offset):
    hidden = jnp.einsum("bsc,cf->bsf", normed, weight, preferred_element_type=jnp.float32) + offset
    return jax.nn.gelu(hidden, approximate=False).astype(jnp.bfloat16)


def solution(mesh):
    row_spec = P("data", "seq", None)
    vec_spec = P(None)
    mat_spec = P(None, None)
    in_specs = (row_spec, vec_spec, vec_spec, mat_spec, vec_spec, vec_spec, vec_spec, mat_spec, vec_spec, mat_spec, vec_spec)

    def per_device(patches, ln1_gain, ln1_bias, w_in, b_in, ln2_gain, ln2_bias, w_spatial, b_spatial, w_out, b_out):
        half_dim = w_out.shape[0]
        images = lax.all_to_all(patches, "seq", 0, 1, tiled=True)
        normed = layer_norm(images, ln1_gain, ln1_bias)
        gate_a = gelu_proj(normed, w_in[:, :half_dim], b_in[:half_dim])
        gate_n = layer_norm(gelu_proj(normed, w_in[:, half_dim:], b_in[half_dim:]), ln2_gain, ln2_bias)
        spatial = jnp.einsum("rs,bre->bse", w_spatial, gate_n, preferred_element_type=jnp.float32).astype(jnp.bfloat16)
        gated = (gate_a.astype(jnp.float32) * (spatial.astype(jnp.float32) + b_spatial[:, None])).astype(jnp.bfloat16)
        mixed = jnp.einsum("bse,ec->bsc", gated, w_out, preferred_element_type=jnp.float32) + b_out
        result = (images.astype(jnp.float32) + mixed).astype(jnp.bfloat16)
        return lax.all_to_all(result, "seq", 1, 0, tiled=True)

    return jax.shard_map(per_device, mesh=mesh, in_specs=in_specs, out_specs=row_spec, check_vma=False)
```

```python
import functools

import jax
import jax.numpy as jnp
from jax import lax
from jax.experimental import pallas as pl
from jax.experimental.pallas import tpu as pltpu
from jax.sharding import PartitionSpec as P

LN_EPS = 1e-6
MESH = pl.DeviceIdType.MESH
SQRT_HALF = 0.7071067811865476


def normalize(values_f, gain_vec, offset):
    mean_val = jnp.mean(values_f, axis=-1, keepdims=True)
    centered = values_f - mean_val
    var_val = jnp.mean(centered * centered, axis=-1, keepdims=True)
    return (centered * lax.rsqrt(var_val + LN_EPS) * gain_vec + offset).astype(jnp.bfloat16)


def kernel(n, row_tile, col_tile, x_hbm, g1_hbm, b1_hbm, wi_hbm, bi_hbm, g2_hbm, b2_hbm, ws_hbm, bs_hbm, wo_hbm, bo_hbm,
           out_hbm, gath, ybuf, hbuf, nbuf, gbuf, g1, b1, wi, bi, g2, b2, ws, wst, bs, bst, wo, bo,
           w_sem, in_send, in_recv, out_send, out_recv):
    me = lax.axis_index("seq")
    per_dev, rows, chans = x_hbm.shape[1], x_hbm.shape[2], x_hbm.shape[3]
    patches = n * rows
    half = wo.shape[0]
    bf16, f32 = jnp.bfloat16, jnp.float32

    def partner(k):
        step = lax.div(k + 1, 2) * (2 * lax.rem(k, 2) - 1)
        return lax.rem(me + step + n, n)

    loads = [pltpu.make_async_copy(src, dst, w_sem.at[i]) for i, (src, dst) in enumerate((
        (g1_hbm, g1), (b1_hbm, b1), (wi_hbm, wi), (bi_hbm, bi), (g2_hbm, g2), (b2_hbm, b2),
        (ws_hbm, ws), (bs_hbm, bs), (wo_hbm, wo), (bo_hbm, bo)))]
    for load in loads:
        load.start()

    barrier = pltpu.get_barrier_semaphore()

    def greet(k, carry):
        pl.semaphore_signal(barrier, inc=1, device_id={"seq": partner(k)}, device_id_type=MESH)
        return carry

    lax.fori_loop(1, n, greet, 0)
    pl.semaphore_wait(barrier, n - 1)

    def mine(base):
        return pl.ds(pl.multiple_of(base * patches + me * rows, rows), rows)

    def send_in(i, carry):
        j, k = lax.div(i, n - 1), lax.rem(i, n - 1) + 1
        to = partner(k)
        pltpu.make_async_remote_copy(
            src_ref=x_hbm.at[to, j], dst_ref=gath.at[mine(j)], send_sem=in_send.at[0], recv_sem=in_recv.at[j],
            device_id={"seq": to}, device_id_type=MESH).start()
        return carry

    lax.fori_loop(0, per_dev * (n - 1), send_in, 0)
    for j in range(per_dev):
        pltpu.make_async_copy(x_hbm.at[me, j], gath.at[mine(j)], in_recv.at[j]).start()

    for load in loads:
        load.wait()
    wst[...] = jnp.transpose(ws[...].astype(f32)).astype(bf16)
    bst[...] = jnp.transpose(jnp.broadcast_to(bs[...], (128, patches)))

    def one_image(j, carry):
        base = pl.multiple_of(j * patches, patches)
        image = gath.at[pl.ds(base, patches)]
        pltpu.make_async_copy(image, image, in_recv.at[j]).wait()

        def project(r, carry):
            start = pl.multiple_of(r * row_tile, row_tile)
            sl = pl.ds(start, row_tile)
            u = normalize(gath[pl.ds(pl.multiple_of(base + start, row_tile), row_tile), :].astype(f32), g1[...], b1[...])

            def column(c, carry):
                cs = pl.ds(pl.multiple_of(c * col_tile, col_tile), col_tile)
                hidden = jnp.dot(u, wi[:, cs], preferred_element_type=f32) + bi[:, cs]
                hbuf[sl, cs] = (0.5 * hidden * (1.0 + lax.erf(hidden * SQRT_HALF))).astype(bf16)
                return carry

            lax.fori_loop(0, 2 * half // col_tile, column, 0)

            def norm2(q, carry):
                qs = pl.ds(pl.multiple_of(start + q * 32, 32), 32)
                nbuf[qs, :] = normalize(hbuf[qs, half:].astype(f32), g2[...], b2[...])
                return carry

            lax.fori_loop(0, row_tile // 32, norm2, 0)
            return carry

        lax.fori_loop(0, patches // row_tile, project, 0)

        def mix(r, carry):
            start = pl.multiple_of(r * row_tile, row_tile)
            sl = pl.ds(start, row_tile)
            ysl = pl.ds(pl.multiple_of(base + start, row_tile), row_tile)
            bias = jnp.concatenate([bst[sl, :]] * (col_tile // 128), axis=1)

            def column(c, carry):
                cs = pl.ds(pl.multiple_of(c * col_tile, col_tile), col_tile)
                s = jnp.dot(wst[sl, :], nbuf[:, cs], preferred_element_type=f32).astype(bf16).astype(f32)
                gbuf[:, cs] = (hbuf[sl, cs].astype(f32) * (s + bias)).astype(bf16)
                return carry

            lax.fori_loop(0, half // col_tile, column, 0)
            mixed = jnp.dot(gbuf[...], wo[...], preferred_element_type=f32) + bo[...]
            ybuf[ysl, :] = (gath[ysl, :].astype(f32) + mixed).astype(bf16)
            return carry

        lax.fori_loop(0, patches // row_tile, mix, 0)

        def rows_of(dev):
            return pl.ds(pl.multiple_of(base + dev * rows, rows), rows)

        def send_out(k, carry):
            to = partner(k)
            pltpu.make_async_remote_copy(
                src_ref=ybuf.at[rows_of(to)], dst_ref=out_hbm.at[me, j], send_sem=out_send.at[0], recv_sem=out_recv.at[0],
                device_id={"seq": to}, device_id_type=MESH).start()
            return carry

        lax.fori_loop(1, n, send_out, 0)
        pltpu.make_async_copy(ybuf.at[rows_of(me)], out_hbm.at[me, j], out_recv.at[0]).start()
        return carry

    lax.fori_loop(0, per_dev, one_image, 0)

    sent = pl.ds(0, per_dev * (n - 1) * rows)
    pltpu.make_async_copy(ybuf.at[sent], ybuf.at[sent], in_send.at[0]).wait()
    pltpu.make_async_copy(ybuf.at[sent], ybuf.at[sent], out_send.at[0]).wait()
    pltpu.make_async_copy(out_hbm, out_hbm, out_recv.at[0]).wait()


def solution(mesh):
    row_spec = P("data", "seq", None)
    vec_spec = P(None)
    mat_spec = P(None, None)
    in_specs = (row_spec, vec_spec, vec_spec, mat_spec, vec_spec, vec_spec, vec_spec, mat_spec, vec_spec, mat_spec, vec_spec)
    n = mesh.shape["seq"]

    def per_device(patches, ln1_gain, ln1_bias, w_in, b_in, ln2_gain, ln2_bias, w_spatial, b_spatial, w_out, b_out):
        images, rows, chans = patches.shape
        half = w_out.shape[0]
        per_dev = images // n
        total = n * rows
        row_tile, col_tile = 256, 512
        bf16, f32 = jnp.bfloat16, jnp.float32
        dma, vmem = pltpu.SemaphoreType.DMA, pltpu.VMEM
        out = pl.pallas_call(
            functools.partial(kernel, n, row_tile, col_tile),
            out_shape=jax.ShapeDtypeStruct((n, per_dev, rows, chans), bf16),
            in_specs=[pl.BlockSpec(memory_space=pltpu.HBM)] * 11,
            out_specs=pl.BlockSpec(memory_space=pltpu.HBM),
            scratch_shapes=[
                vmem((per_dev * total, chans), bf16),
                vmem((per_dev * total, chans), bf16),
                vmem((total, 2 * half), bf16),
                vmem((total, half), bf16),
                vmem((row_tile, half), bf16),
                vmem((1, chans), f32), vmem((1, chans), f32),
                vmem((chans, 2 * half), bf16), vmem((1, 2 * half), f32),
                vmem((1, half), f32), vmem((1, half), f32),
                vmem((total, total), bf16), vmem((total, total), bf16),
                vmem((1, total), f32), vmem((total, 128), f32),
                vmem((half, chans), bf16), vmem((1, chans), f32),
                dma((10,)), dma((1,)), dma((per_dev,)), dma((1,)), dma((1,)),
            ],
            compiler_params=pltpu.CompilerParams(
                collective_id=0, has_side_effects=True, vmem_limit_bytes=56 * 1024 * 1024),
            name="gmlp",
        )(patches.reshape(n, per_dev, rows, chans), ln1_gain[None], ln1_bias[None], w_in, b_in[None],
          ln2_gain[None], ln2_bias[None], w_spatial, b_spatial[None], w_out, b_out[None])
        return out.reshape(images, rows, chans)

    return jax.shard_map(per_device, mesh=mesh, in_specs=in_specs, out_specs=row_spec, check_vma=False)
```

```python
import functools

import jax
import jax.numpy as jnp
from jax import lax
from jax.experimental import pallas as pl
from jax.experimental.pallas import tpu as pltpu
from jax.sharding import PartitionSpec as P

LN_EPS = 1e-6
MESH = pl.DeviceIdType.MESH
SQRT_HALF = 0.7071067811865476


def normalize(values_f, gain_vec, offset):
    mean_val = jnp.mean(values_f, axis=-1, keepdims=True)
    centered = values_f - mean_val
    var_val = jnp.mean(centered * centered, axis=-1, keepdims=True)
    return (centered * lax.rsqrt(var_val + LN_EPS) * gain_vec + offset).astype(jnp.bfloat16)


def kernel(n, row_tile, col_tile, x_hbm, g1_hbm, b1_hbm, wi_hbm, bi_hbm, g2_hbm, b2_hbm, ws_hbm, bs_hbm, wo_hbm, bo_hbm,
           out_ref, gath, ybuf, hbuf, nbuf, gbuf, g1, b1, wi, bi, g2, b2, ws, wst, bs, bst, wo, bo,
           w_sem, in_send, in_recv, out_send, out_recv):
    me = lax.axis_index("seq")
    per_dev, rows, chans = x_hbm.shape[1], x_hbm.shape[2], x_hbm.shape[3]
    patches = n * rows
    half = wo.shape[0]
    bf16, f32 = jnp.bfloat16, jnp.float32

    chips = n // 2
    chip, core = lax.div(me, 2), lax.rem(me, 2)

    def others(steps):
        found = []
        for step in steps:
            there = 2 * lax.rem(chip + step + chips, chips)
            found += [there + core, there + 1 - core]
        return found + [2 * chip + 1 - core]

    pairs = [(step, -step) for step in range(chips // 2 - 1, 0, -1)]
    out_steps = [chips // 2, *sum(pairs, ())]
    in_steps = [chips // 2, *sum(pairs[-1:] + pairs[:-1], ())]

    loads = [pltpu.make_async_copy(src, dst, w_sem.at[i]) for i, (src, dst) in enumerate((
        (g1_hbm, g1), (b1_hbm, b1), (wi_hbm, wi), (bi_hbm, bi), (g2_hbm, g2), (b2_hbm, b2),
        (ws_hbm, ws), (bs_hbm, bs), (wo_hbm, wo), (bo_hbm, bo)))]
    for load in loads:
        load.start()

    barrier = pltpu.get_barrier_semaphore()

    for to in others(in_steps):
        pl.semaphore_signal(barrier, inc=1, device_id={"seq": to}, device_id_type=MESH)
    pl.semaphore_wait(barrier, n - 1)

    def mine(base):
        return pl.ds(pl.multiple_of(base * patches + me * rows, rows), rows)

    def send_in(j, carry):
        for to in others(in_steps):
            pltpu.make_async_remote_copy(
                src_ref=x_hbm.at[to, j], dst_ref=gath.at[mine(j)], send_sem=in_send.at[0], recv_sem=in_recv.at[j],
                device_id={"seq": to}, device_id_type=MESH).start()
        return carry

    lax.fori_loop(0, per_dev, send_in, 0)
    for j in range(per_dev):
        pltpu.make_async_copy(x_hbm.at[me, j], gath.at[mine(j)], in_recv.at[j]).start()

    for load in loads:
        load.wait()
    wst[...] = jnp.transpose(ws[...].astype(f32)).astype(bf16)
    bst[...] = jnp.transpose(jnp.broadcast_to(bs[...], (128, patches)))

    def one_image(j, carry):
        base = pl.multiple_of(j * patches, patches)
        image = gath.at[pl.ds(base, patches)]
        pltpu.make_async_copy(image, image, in_recv.at[j]).wait()

        def project(r, carry):
            start = pl.multiple_of(r * row_tile, row_tile)
            sl = pl.ds(start, row_tile)
            u = normalize(gath[pl.ds(pl.multiple_of(base + start, row_tile), row_tile), :].astype(f32), g1[...], b1[...])

            def column(c, carry):
                cs = pl.ds(pl.multiple_of(c * col_tile, col_tile), col_tile)
                hidden = jnp.dot(u, wi[:, cs], preferred_element_type=f32) + bi[:, cs]
                hbuf[sl, cs] = (0.5 * hidden * (1.0 + lax.erf(hidden * SQRT_HALF))).astype(bf16)
                return carry

            lax.fori_loop(0, 2 * half // col_tile, column, 0)

            def norm2(q, carry):
                qs = pl.ds(pl.multiple_of(start + q * 32, 32), 32)
                nbuf[qs, :] = normalize(hbuf[qs, half:].astype(f32), g2[...].reshape(1, half), b2[...].reshape(1, half))
                return carry

            lax.fori_loop(0, row_tile // 32, norm2, 0)
            return carry

        lax.fori_loop(0, patches // row_tile, project, 0)

        def mix(r, carry):
            start = pl.multiple_of(r * row_tile, row_tile)
            sl = pl.ds(start, row_tile)
            ysl = pl.ds(pl.multiple_of(base + start, row_tile), row_tile)
            bias = jnp.concatenate([bst[sl, :]] * (col_tile // 128), axis=1)

            def column(c, carry):
                cs = pl.ds(pl.multiple_of(c * col_tile, col_tile), col_tile)
                s = jnp.dot(wst[sl, :], nbuf[:, cs], preferred_element_type=f32).astype(bf16).astype(f32)
                gbuf[:, cs] = (hbuf[sl, cs].astype(f32) * (s + bias)).astype(bf16)
                return carry

            lax.fori_loop(0, half // col_tile, column, 0)
            mixed = jnp.dot(gbuf[...], wo[...], preferred_element_type=f32) + bo[...]
            ybuf[ysl, :] = (gath[ysl, :].astype(f32) + mixed).astype(bf16)
            return carry

        lax.fori_loop(0, patches // row_tile, mix, 0)

        def rows_of(dev):
            return pl.ds(pl.multiple_of(base + dev * rows, rows), rows)

        for to in others(out_steps):
            pltpu.make_async_remote_copy(
                src_ref=ybuf.at[rows_of(to)], dst_ref=out_ref.at[me, j], send_sem=out_send.at[0], recv_sem=out_recv.at[0],
                device_id={"seq": to}, device_id_type=MESH).start()
        pltpu.make_async_copy(ybuf.at[rows_of(me)], out_ref.at[me, j], out_recv.at[0]).start()
        return carry

    lax.fori_loop(0, per_dev, one_image, 0)

    sent = pl.ds(0, per_dev * (n - 1) * rows)
    pltpu.make_async_copy(ybuf.at[sent], ybuf.at[sent], in_send.at[0]).wait()
    pltpu.make_async_copy(ybuf.at[sent], ybuf.at[sent], out_send.at[0]).wait()
    pltpu.make_async_copy(out_ref, out_ref, out_recv.at[0]).wait()


def solution(mesh):
    row_spec = P("data", "seq", None)
    vec_spec = P(None)
    mat_spec = P(None, None)
    in_specs = (row_spec, vec_spec, vec_spec, mat_spec, vec_spec, vec_spec, vec_spec, mat_spec, vec_spec, mat_spec, vec_spec)
    n = mesh.shape["seq"]

    def per_device(patches, ln1_gain, ln1_bias, w_in, b_in, ln2_gain, ln2_bias, w_spatial, b_spatial, w_out, b_out):
        images, rows, chans = patches.shape
        half = w_out.shape[0]
        per_dev = images // n
        total = n * rows
        row_tile, col_tile = 256, 512
        bf16, f32 = jnp.bfloat16, jnp.float32
        dma, vmem = pltpu.SemaphoreType.DMA, pltpu.VMEM
        out = pl.pallas_call(
            functools.partial(kernel, n, row_tile, col_tile),
            out_shape=pltpu.VMEM((n, per_dev, rows, chans), bf16),
            in_specs=[pl.BlockSpec(memory_space=pltpu.HBM)] * 11,
            out_specs=pl.BlockSpec(memory_space=pltpu.VMEM),
            scratch_shapes=[
                vmem((per_dev * total, chans), bf16),
                vmem((per_dev * total, chans), bf16),
                vmem((total, 2 * half), bf16),
                vmem((total, half), bf16),
                vmem((row_tile, half), bf16),
                vmem((1, chans), f32), vmem((1, chans), f32),
                vmem((chans, 2 * half), bf16), vmem((1, 2 * half), f32),
                vmem((half,), f32), vmem((half,), f32),
                vmem((total, total), bf16), vmem((total, total), bf16),
                vmem((1, total), f32), vmem((total, 128), f32),
                vmem((half, chans), bf16), vmem((1, chans), f32),
                dma((10,)), dma((1,)), dma((per_dev,)), dma((1,)), dma((1,)),
            ],
            compiler_params=pltpu.CompilerParams(
                collective_id=0, has_side_effects=True, vmem_limit_bytes=56 * 1024 * 1024),
            name="gmlp",
        )(patches.reshape(n, per_dev, rows, chans), ln1_gain[None], ln1_bias[None], w_in, b_in[None],
          ln2_gain, ln2_bias, w_spatial, b_spatial[None], w_out, b_out[None])
        return out.reshape(images, rows, chans)

    return jax.shard_map(per_device, mesh=mesh, in_specs=in_specs, out_specs=row_spec, check_vma=False)
```

```python
import functools

import jax
import jax.numpy as jnp
from jax import lax
from jax.experimental import pallas as pl
from jax.experimental.pallas import tpu as pltpu
from jax.sharding import PartitionSpec as P

LN_EPS = 1e-6
MESH = pl.DeviceIdType.MESH
SQRT_HALF = 0.7071067811865476


def normalize(values_f, gain_vec, offset):
    mean_val = jnp.mean(values_f, axis=-1, keepdims=True)
    centered = values_f - mean_val
    var_val = jnp.mean(centered * centered, axis=-1, keepdims=True)
    return (centered * lax.rsqrt(var_val + LN_EPS) * gain_vec + offset).astype(jnp.bfloat16)


def kernel(n, row_tile, col_tile, x_hbm, g1_hbm, b1_hbm, wi_hbm, bi_hbm, g2_hbm, b2_hbm, ws_hbm, bs_hbm, wo_hbm, bo_hbm,
           out_ref, gath, ybuf, hbuf, nbuf, gbuf, g1, b1, wi, bi, g2, b2, ws, wst, bs, bst, wo, bo,
           w_sem, in_send, in_recv, out_send, out_recv):
    me = lax.axis_index("seq")
    per_dev, rows, chans = x_hbm.shape[1], x_hbm.shape[2], x_hbm.shape[3]
    patches = n * rows
    half = wo.shape[0]
    bf16, f32 = jnp.bfloat16, jnp.float32

    def others(first):
        place = lax.rem(me - first + n, n)
        return [lax.rem(first + i + (place <= i).astype(jnp.int32), n) for i in range(n - 1)]

    loads = [pltpu.make_async_copy(src, dst, w_sem.at[i]) for i, (src, dst) in enumerate((
        (g1_hbm, g1), (b1_hbm, b1), (wi_hbm, wi), (bi_hbm, bi), (g2_hbm, g2), (b2_hbm, b2),
        (ws_hbm, ws), (bs_hbm, bs), (wo_hbm, wo), (bo_hbm, bo)))]
    for load in loads:
        load.start()

    barrier = pltpu.get_barrier_semaphore()

    for to in others(0):
        pl.semaphore_signal(barrier, inc=1, device_id={"seq": to}, device_id_type=MESH)
    pl.semaphore_wait(barrier, n - 1)

    def mine(base):
        return pl.ds(pl.multiple_of(base * patches + me * rows, rows), rows)

    def send_in(j, carry):
        for to in others(n // 2):
            pltpu.make_async_remote_copy(
                src_ref=x_hbm.at[to, j], dst_ref=gath.at[mine(j)], send_sem=in_send.at[0], recv_sem=in_recv.at[j],
                device_id={"seq": to}, device_id_type=MESH).start()
        return carry

    lax.fori_loop(0, per_dev, send_in, 0)
    for j in range(per_dev):
        pltpu.make_async_copy(x_hbm.at[me, j], gath.at[mine(j)], in_recv.at[j]).start()

    for load in loads:
        load.wait()
    wst[...] = jnp.transpose(ws[...].astype(f32)).astype(bf16)
    bst[...] = jnp.transpose(jnp.broadcast_to(bs[...], (128, patches)))

    def one_image(j, carry):
        base = pl.multiple_of(j * patches, patches)
        image = gath.at[pl.ds(base, patches)]
        pltpu.make_async_copy(image, image, in_recv.at[j]).wait()

        def project(r, carry):
            start = pl.multiple_of(r * row_tile, row_tile)
            sl = pl.ds(start, row_tile)
            u = normalize(gath[pl.ds(pl.multiple_of(base + start, row_tile), row_tile), :].astype(f32), g1[...], b1[...])

            def column(c, carry):
                cs = pl.ds(pl.multiple_of(c * col_tile, col_tile), col_tile)
                hidden = jnp.dot(u, wi[:, cs], preferred_element_type=f32) + bi[:, cs]
                hbuf[sl, cs] = (0.5 * hidden * (1.0 + lax.erf(hidden * SQRT_HALF))).astype(bf16)
                return carry

            lax.fori_loop(0, 2 * half // col_tile, column, 0)

            def norm2(q, carry):
                qs = pl.ds(pl.multiple_of(start + q * 32, 32), 32)
                nbuf[qs, :] = normalize(hbuf[qs, half:].astype(f32), g2[...].reshape(1, half), b2[...].reshape(1, half))
                return carry

            lax.fori_loop(0, row_tile // 32, norm2, 0)
            return carry

        lax.fori_loop(0, patches // row_tile, project, 0)

        def mix(r, carry):
            start = pl.multiple_of(r * row_tile, row_tile)
            sl = pl.ds(start, row_tile)
            ysl = pl.ds(pl.multiple_of(base + start, row_tile), row_tile)
            bias = jnp.concatenate([bst[sl, :]] * (col_tile // 128), axis=1)

            def column(c, carry):
                cs = pl.ds(pl.multiple_of(c * col_tile, col_tile), col_tile)
                s = jnp.dot(wst[sl, :], nbuf[:, cs], preferred_element_type=f32).astype(bf16).astype(f32)
                gbuf[:, cs] = (hbuf[sl, cs].astype(f32) * (s + bias)).astype(bf16)
                return carry

            lax.fori_loop(0, half // col_tile, column, 0)
            mixed = jnp.dot(gbuf[...], wo[...], preferred_element_type=f32) + bo[...]
            ybuf[ysl, :] = (gath[ysl, :].astype(f32) + mixed).astype(bf16)
            return carry

        lax.fori_loop(0, patches // row_tile, mix, 0)

        def rows_of(dev):
            return pl.ds(pl.multiple_of(base + dev * rows, rows), rows)

        for to in others(0):
            pltpu.make_async_remote_copy(
                src_ref=ybuf.at[rows_of(to)], dst_ref=out_ref.at[me, j], send_sem=out_send.at[0], recv_sem=out_recv.at[0],
                device_id={"seq": to}, device_id_type=MESH).start()
        pltpu.make_async_copy(ybuf.at[rows_of(me)], out_ref.at[me, j], out_recv.at[0]).start()
        return carry

    lax.fori_loop(0, per_dev, one_image, 0)

    sent = pl.ds(0, per_dev * (n - 1) * rows)
    pltpu.make_async_copy(ybuf.at[sent], ybuf.at[sent], in_send.at[0]).wait()
    pltpu.make_async_copy(ybuf.at[sent], ybuf.at[sent], out_send.at[0]).wait()
    pltpu.make_async_copy(out_ref, out_ref, out_recv.at[0]).wait()


def solution(mesh):
    row_spec = P("data", "seq", None)
    vec_spec = P(None)
    mat_spec = P(None, None)
    in_specs = (row_spec, vec_spec, vec_spec, mat_spec, vec_spec, vec_spec, vec_spec, mat_spec, vec_spec, mat_spec, vec_spec)
    n = mesh.shape["seq"]

    def per_device(patches, ln1_gain, ln1_bias, w_in, b_in, ln2_gain, ln2_bias, w_spatial, b_spatial, w_out, b_out):
        images, rows, chans = patches.shape
        half = w_out.shape[0]
        per_dev = images // n
        total = n * rows
        row_tile, col_tile = 256, 512
        bf16, f32 = jnp.bfloat16, jnp.float32
        dma, vmem = pltpu.SemaphoreType.DMA, pltpu.VMEM
        out = pl.pallas_call(
            functools.partial(kernel, n, row_tile, col_tile),
            out_shape=pltpu.VMEM((n, per_dev, rows, chans), bf16),
            in_specs=[pl.BlockSpec(memory_space=pltpu.HBM)] * 11,
            out_specs=pl.BlockSpec(memory_space=pltpu.VMEM),
            scratch_shapes=[
                vmem((per_dev * total, chans), bf16),
                vmem((per_dev * total, chans), bf16),
                vmem((total, 2 * half), bf16),
                vmem((total, half), bf16),
                vmem((row_tile, half), bf16),
                vmem((1, chans), f32), vmem((1, chans), f32),
                vmem((chans, 2 * half), bf16), vmem((1, 2 * half), f32),
                vmem((half,), f32), vmem((half,), f32),
                vmem((total, total), bf16), vmem((total, total), bf16),
                vmem((1, total), f32), vmem((total, 128), f32),
                vmem((half, chans), bf16), vmem((1, chans), f32),
                dma((10,)), dma((1,)), dma((per_dev,)), dma((1,)), dma((1,)),
            ],
            compiler_params=pltpu.CompilerParams(
                collective_id=0, has_side_effects=True, vmem_limit_bytes=56 * 1024 * 1024),
            name="gmlp",
        )(patches.reshape(n, per_dev, rows, chans), ln1_gain[None], ln1_bias[None], w_in, b_in[None],
          ln2_gain, ln2_bias, w_spatial, b_spatial[None], w_out, b_out[None])
        return out.reshape(images, rows, chans)

    return jax.shard_map(per_device, mesh=mesh, in_specs=in_specs, out_specs=row_spec, check_vma=False)
```

```python
import functools

import jax
import jax.numpy as jnp
from jax import lax
from jax.experimental import pallas as pl
from jax.experimental.pallas import tpu as pltpu
from jax.sharding import PartitionSpec as P

LN_EPS = 1e-6
MESH = pl.DeviceIdType.MESH
SQRT_HALF = 0.7071067811865476


def normalize(values_f, gain_vec, offset):
    mean_val = jnp.mean(values_f, axis=-1, keepdims=True)
    centered = values_f - mean_val
    var_val = jnp.mean(centered * centered, axis=-1, keepdims=True)
    return (centered * lax.rsqrt(var_val + LN_EPS) * gain_vec + offset).astype(jnp.bfloat16)


def kernel(n, row_tile, col_tile, x_hbm, g1_hbm, b1_hbm, wi_hbm, bi_hbm, g2_hbm, b2_hbm, ws_hbm, bs_hbm, wo_hbm, bo_hbm,
           out_ref, gath, ybuf, hbuf, nbuf, gbuf, g1, b1, wi, bi, g2, b2, ws, wst, bs, bst, wo, bo,
           answered, complete, w_sem, in_send, in_recv, out_send, out_recv):
    me = lax.axis_index("seq")
    per_dev, rows, chans = x_hbm.shape[1], x_hbm.shape[2], x_hbm.shape[3]
    patches = n * rows
    half = wo.shape[0]
    bf16, f32 = jnp.bfloat16, jnp.float32

    chips = n // 2
    chip, core = lax.div(me, 2), lax.rem(me, 2)

    def by_distance():
        found = []
        for step in [chips // 2, *sum(((step, -step) for step in range(chips // 2 - 1, 0, -1)), ())]:
            there = 2 * lax.rem(chip + step + chips, chips)
            found += [there + core, there + 1 - core]
        return found + [2 * chip + 1 - core]

    def by_index():
        return [i + (me <= i).astype(jnp.int32) for i in range(n - 1)]

    loads = [pltpu.make_async_copy(src, dst, w_sem.at[i]) for i, (src, dst) in enumerate((
        (g1_hbm, g1), (b1_hbm, b1), (wi_hbm, wi), (bi_hbm, bi), (g2_hbm, g2), (b2_hbm, b2),
        (ws_hbm, ws), (bs_hbm, bs), (wo_hbm, wo), (bo_hbm, bo)))]
    for load in loads:
        load.start()

    def mine(base):
        return pl.ds(pl.multiple_of(base * patches + me * rows, rows), rows)

    def send_in(j, to):
        pltpu.make_async_remote_copy(
            src_ref=x_hbm.at[to, j], dst_ref=gath.at[mine(j)], send_sem=in_send.at[0], recv_sem=in_recv.at[j],
            device_id={"seq": to}, device_id_type=MESH).start()

    barrier = pltpu.get_barrier_semaphore()
    span = n // 2
    low = me < span
    early = per_dev // 2

    def tell(sem, to):
        pl.semaphore_signal(sem, inc=1, device_id={"seq": to}, device_id_type=MESH)

    def send_early(first):
        for j in range(early):
            for to in range(first, first + span):
                @pl.when(me != to)
                def _():
                    send_in(j, to)

    @pl.when(low)
    def _():
        for to in by_index():
            tell(barrier, to)

    pl.semaphore_wait(barrier, span - low.astype(jnp.int32))

    @pl.when(jnp.logical_not(low))
    def _():
        for to in range(span):
            tell(answered, to)

    send_early(0)

    @pl.when(low)
    def _():
        pl.semaphore_wait(answered, span)
        tell(complete, n - 1 - me)

    @pl.when(jnp.logical_not(low))
    def _():
        pl.semaphore_wait(complete, 1)

    send_early(span)

    def send_late(j, carry):
        for to in by_distance():
            send_in(j, to)
        return carry

    lax.fori_loop(early, per_dev, send_late, 0)
    for j in range(per_dev):
        pltpu.make_async_copy(x_hbm.at[me, j], gath.at[mine(j)], in_recv.at[j]).start()

    for load in loads:
        load.wait()
    wst[...] = jnp.transpose(ws[...].astype(f32)).astype(bf16)
    bst[...] = jnp.transpose(jnp.broadcast_to(bs[...], (128, patches)))

    def one_image(j, carry):
        base = pl.multiple_of(j * patches, patches)
        image = gath.at[pl.ds(base, patches)]
        pltpu.make_async_copy(image, image, in_recv.at[j]).wait()

        def project(r, carry):
            start = pl.multiple_of(r * row_tile, row_tile)
            sl = pl.ds(start, row_tile)
            u = normalize(gath[pl.ds(pl.multiple_of(base + start, row_tile), row_tile), :].astype(f32), g1[...], b1[...])

            def column(c, carry):
                cs = pl.ds(pl.multiple_of(c * col_tile, col_tile), col_tile)
                hidden = jnp.dot(u, wi[:, cs], preferred_element_type=f32) + bi[:, cs]
                hbuf[sl, cs] = (0.5 * hidden * (1.0 + lax.erf(hidden * SQRT_HALF))).astype(bf16)
                return carry

            lax.fori_loop(0, 2 * half // col_tile, column, 0)

            def norm2(q, carry):
                qs = pl.ds(pl.multiple_of(start + q * 32, 32), 32)
                nbuf[qs, :] = normalize(hbuf[qs, half:].astype(f32), g2[...].reshape(1, half), b2[...].reshape(1, half))
                return carry

            lax.fori_loop(0, row_tile // 32, norm2, 0)
            return carry

        lax.fori_loop(0, patches // row_tile, project, 0)

        def mix(r, carry):
            start = pl.multiple_of(r * row_tile, row_tile)
            sl = pl.ds(start, row_tile)
            ysl = pl.ds(pl.multiple_of(base + start, row_tile), row_tile)
            bias = jnp.concatenate([bst[sl, :]] * (col_tile // 128), axis=1)

            def column(c, carry):
                cs = pl.ds(pl.multiple_of(c * col_tile, col_tile), col_tile)
                s = jnp.dot(wst[sl, :], nbuf[:, cs], preferred_element_type=f32).astype(bf16).astype(f32)
                gbuf[:, cs] = (hbuf[sl, cs].astype(f32) * (s + bias)).astype(bf16)
                return carry

            lax.fori_loop(0, half // col_tile, column, 0)
            mixed = jnp.dot(gbuf[...], wo[...], preferred_element_type=f32) + bo[...]
            ybuf[ysl, :] = (gath[ysl, :].astype(f32) + mixed).astype(bf16)
            return carry

        lax.fori_loop(0, patches // row_tile, mix, 0)

        def rows_of(dev):
            return pl.ds(pl.multiple_of(base + dev * rows, rows), rows)

        def send_out(to):
            pltpu.make_async_remote_copy(
                src_ref=ybuf.at[rows_of(to)], dst_ref=out_ref.at[me, j], send_sem=out_send.at[0], recv_sem=out_recv.at[0],
                device_id={"seq": to}, device_id_type=MESH).start()

        last = j == per_dev - 1
        for far, low in zip(by_distance(), by_index()):
            send_out(jnp.where(last, low, far))
        pltpu.make_async_copy(ybuf.at[rows_of(me)], out_ref.at[me, j], out_recv.at[0]).start()
        return carry

    lax.fori_loop(0, per_dev, one_image, 0)

    sent = pl.ds(0, per_dev * (n - 1) * rows)
    pltpu.make_async_copy(ybuf.at[sent], ybuf.at[sent], in_send.at[0]).wait()
    pltpu.make_async_copy(ybuf.at[sent], ybuf.at[sent], out_send.at[0]).wait()
    pltpu.make_async_copy(out_ref, out_ref, out_recv.at[0]).wait()


def solution(mesh):
    row_spec = P("data", "seq", None)
    vec_spec = P(None)
    mat_spec = P(None, None)
    in_specs = (row_spec, vec_spec, vec_spec, mat_spec, vec_spec, vec_spec, vec_spec, mat_spec, vec_spec, mat_spec, vec_spec)
    n = mesh.shape["seq"]

    def per_device(patches, ln1_gain, ln1_bias, w_in, b_in, ln2_gain, ln2_bias, w_spatial, b_spatial, w_out, b_out):
        images, rows, chans = patches.shape
        half = w_out.shape[0]
        per_dev = images // n
        total = n * rows
        row_tile, col_tile = 256, 512
        bf16, f32 = jnp.bfloat16, jnp.float32
        dma, vmem = pltpu.SemaphoreType.DMA, pltpu.VMEM
        out = pl.pallas_call(
            functools.partial(kernel, n, row_tile, col_tile),
            out_shape=pltpu.VMEM((n, per_dev, rows, chans), bf16),
            in_specs=[pl.BlockSpec(memory_space=pltpu.HBM)] * 11,
            out_specs=pl.BlockSpec(memory_space=pltpu.VMEM),
            scratch_shapes=[
                vmem((per_dev * total, chans), bf16),
                vmem((per_dev * total, chans), bf16),
                vmem((total, 2 * half), bf16),
                vmem((total, half), bf16),
                vmem((row_tile, half), bf16),
                vmem((1, chans), f32), vmem((1, chans), f32),
                vmem((chans, 2 * half), bf16), vmem((1, 2 * half), f32),
                vmem((half,), f32), vmem((half,), f32),
                vmem((total, total), bf16), vmem((total, total), bf16),
                vmem((1, total), f32), vmem((total, 128), f32),
                vmem((half, chans), bf16), vmem((1, chans), f32),
                pltpu.SemaphoreType.REGULAR, pltpu.SemaphoreType.REGULAR,
                dma((10,)), dma((1,)), dma((per_dev,)), dma((1,)), dma((1,)),
            ],
            compiler_params=pltpu.CompilerParams(
                collective_id=0, has_side_effects=True, vmem_limit_bytes=56 * 1024 * 1024),
            name="gmlp",
        )(patches.reshape(n, per_dev, rows, chans), ln1_gain[None], ln1_bias[None], w_in, b_in[None],
          ln2_gain, ln2_bias, w_spatial, b_spatial[None], w_out, b_out[None])
        return out.reshape(images, rows, chans)

    return jax.shard_map(per_device, mesh=mesh, in_specs=in_specs, out_specs=row_spec, check_vma=False)
```

```python
import functools

import jax
import jax.numpy as jnp
from jax import lax
from jax.experimental import pallas as pl
from jax.experimental.pallas import tpu as pltpu
from jax.sharding import PartitionSpec as P

LN_EPS = 1e-6
MESH = pl.DeviceIdType.MESH
SQRT_HALF = 0.7071067811865476
GREET_STEPS = (4, 2, -2, 3, -3, 1, -1, 0)
IN_STEPS = (-2, 0, -1, 3, 2, 1, 4, -3)
OUT_STEPS = (4, 3, -3, -1, -2, 1, 0, 2)


def normalize(values_f, gain_vec, offset):
    mean_val = jnp.mean(values_f, axis=-1, keepdims=True)
    centered = values_f - mean_val
    var_val = jnp.mean(centered * centered, axis=-1, keepdims=True)
    return (centered * lax.rsqrt(var_val + LN_EPS) * gain_vec + offset).astype(jnp.bfloat16)


def kernel(n, row_tile, col_tile, x_hbm, g1_hbm, b1_hbm, wi_hbm, bi_hbm, g2_hbm, b2_hbm, ws_hbm, bs_hbm, wo_hbm, bo_hbm,
           out_ref, gath, ybuf, hbuf, nbuf, gbuf, g1, b1, wi, bi, g2, b2, ws, wst, bs, bst, wo, bo,
           answered, complete, w_sem, in_send, in_recv, out_send, out_recv):
    me = lax.axis_index("seq")
    per_dev, rows, chans = x_hbm.shape[1], x_hbm.shape[2], x_hbm.shape[3]
    patches = n * rows
    half = wo.shape[0]
    bf16, f32 = jnp.bfloat16, jnp.float32

    chips = n // 2
    chip, core = lax.div(me, 2), lax.rem(me, 2)

    def ring(steps):
        found = []
        for step in steps:
            there = 2 * lax.rem(chip + step + chips, chips)
            found += [there + core, there + 1 - core] if step else [there + 1 - core]
        assert len(found) == n - 1
        return found

    def by_index():
        return [i + (me <= i).astype(jnp.int32) for i in range(n - 1)]

    loads = [pltpu.make_async_copy(src, dst, w_sem.at[i]) for i, (src, dst) in enumerate((
        (g1_hbm, g1), (b1_hbm, b1), (wi_hbm, wi), (bi_hbm, bi), (g2_hbm, g2), (b2_hbm, b2),
        (ws_hbm, ws), (bs_hbm, bs), (wo_hbm, wo), (bo_hbm, bo)))]

    def mine(base):
        return pl.ds(pl.multiple_of(base * patches + me * rows, rows), rows)

    def send_in(j, to):
        pltpu.make_async_remote_copy(
            src_ref=x_hbm.at[to, j], dst_ref=gath.at[mine(j)], send_sem=in_send.at[0], recv_sem=in_recv.at[j],
            device_id={"seq": to}, device_id_type=MESH).start()

    barrier = pltpu.get_barrier_semaphore()
    span = n // 2
    low = me < span
    early = 2

    def tell(sem, to):
        pl.semaphore_signal(sem, inc=1, device_id={"seq": to}, device_id_type=MESH)

    def send_early(first):
        for j in range(early):
            for to in range(first, first + span):
                @pl.when(me != to)
                def _():
                    send_in(j, to)

    @pl.when(low)
    def _():
        for to in ring(GREET_STEPS):
            tell(barrier, to)

    for load in loads:
        load.start()
    pl.semaphore_wait(barrier, span - low.astype(jnp.int32))

    @pl.when(jnp.logical_not(low))
    def _():
        for to in range(span):
            tell(answered, to)

    send_early(0)

    @pl.when(low)
    def _():
        pl.semaphore_wait(answered, span)
        tell(complete, n - 1 - me)

    @pl.when(jnp.logical_not(low))
    def _():
        pl.semaphore_wait(complete, 1)

    send_early(span)

    def send_late(j, carry):
        for to in ring(IN_STEPS):
            send_in(j, to)
        return carry

    lax.fori_loop(early, per_dev, send_late, 0)
    for j in range(per_dev):
        pltpu.make_async_copy(x_hbm.at[me, j], gath.at[mine(j)], in_recv.at[j]).start()

    for load in loads:
        load.wait()
    wst[...] = jnp.transpose(ws[...].astype(f32)).astype(bf16)
    bst[...] = jnp.transpose(jnp.broadcast_to(bs[...], (128, patches)))

    def one_image(j, carry):
        base = pl.multiple_of(j * patches, patches)
        image = gath.at[pl.ds(base, patches)]
        pltpu.make_async_copy(image, image, in_recv.at[j]).wait()

        def project(r, carry):
            start = pl.multiple_of(r * row_tile, row_tile)
            sl = pl.ds(start, row_tile)
            u = normalize(gath[pl.ds(pl.multiple_of(base + start, row_tile), row_tile), :].astype(f32), g1[...], b1[...])

            def column(c, carry):
                cs = pl.ds(pl.multiple_of(c * col_tile, col_tile), col_tile)
                hidden = jnp.dot(u, wi[:, cs], preferred_element_type=f32) + bi[:, cs]
                hbuf[sl, cs] = (0.5 * hidden * (1.0 + lax.erf(hidden * SQRT_HALF))).astype(bf16)
                return carry

            lax.fori_loop(0, 2 * half // col_tile, column, 0)

            def norm2(q, carry):
                qs = pl.ds(pl.multiple_of(start + q * 32, 32), 32)
                nbuf[qs, :] = normalize(hbuf[qs, half:].astype(f32), g2[...].reshape(1, half), b2[...].reshape(1, half))
                return carry

            lax.fori_loop(0, row_tile // 32, norm2, 0)
            return carry

        lax.fori_loop(0, patches // row_tile, project, 0)

        def mix(r, carry):
            start = pl.multiple_of(r * row_tile, row_tile)
            sl = pl.ds(start, row_tile)
            ysl = pl.ds(pl.multiple_of(base + start, row_tile), row_tile)
            bias = jnp.concatenate([bst[sl, :]] * (col_tile // 128), axis=1)

            def column(c, carry):
                cs = pl.ds(pl.multiple_of(c * col_tile, col_tile), col_tile)
                s = jnp.dot(wst[sl, :], nbuf[:, cs], preferred_element_type=f32).astype(bf16).astype(f32)
                gbuf[:, cs] = (hbuf[sl, cs].astype(f32) * (s + bias)).astype(bf16)
                return carry

            lax.fori_loop(0, half // col_tile, column, 0)
            mixed = jnp.dot(gbuf[...], wo[...], preferred_element_type=f32) + bo[...]
            ybuf[ysl, :] = (gath[ysl, :].astype(f32) + mixed).astype(bf16)
            return carry

        lax.fori_loop(0, patches // row_tile, mix, 0)

        def rows_of(dev):
            return pl.ds(pl.multiple_of(base + dev * rows, rows), rows)

        def send_out(to):
            pltpu.make_async_remote_copy(
                src_ref=ybuf.at[rows_of(to)], dst_ref=out_ref.at[me, j], send_sem=out_send.at[0], recv_sem=out_recv.at[0],
                device_id={"seq": to}, device_id_type=MESH).start()

        last = j == per_dev - 1
        for far, low in zip(ring(OUT_STEPS), by_index()):
            send_out(jnp.where(last, low, far))
        pltpu.make_async_copy(ybuf.at[rows_of(me)], out_ref.at[me, j], out_recv.at[0]).start()
        return carry

    lax.fori_loop(0, per_dev, one_image, 0)

    sent = pl.ds(0, per_dev * (n - 1) * rows)
    pltpu.make_async_copy(ybuf.at[sent], ybuf.at[sent], in_send.at[0]).wait()
    pltpu.make_async_copy(ybuf.at[sent], ybuf.at[sent], out_send.at[0]).wait()
    pltpu.make_async_copy(out_ref, out_ref, out_recv.at[0]).wait()


def solution(mesh):
    row_spec = P("data", "seq", None)
    vec_spec = P(None)
    mat_spec = P(None, None)
    in_specs = (row_spec, vec_spec, vec_spec, mat_spec, vec_spec, vec_spec, vec_spec, mat_spec, vec_spec, mat_spec, vec_spec)
    n = mesh.shape["seq"]

    def per_device(patches, ln1_gain, ln1_bias, w_in, b_in, ln2_gain, ln2_bias, w_spatial, b_spatial, w_out, b_out):
        images, rows, chans = patches.shape
        half = w_out.shape[0]
        per_dev = images // n
        total = n * rows
        row_tile, col_tile = 256, 512
        bf16, f32 = jnp.bfloat16, jnp.float32
        dma, vmem = pltpu.SemaphoreType.DMA, pltpu.VMEM
        out = pl.pallas_call(
            functools.partial(kernel, n, row_tile, col_tile),
            out_shape=pltpu.VMEM((n, per_dev, rows, chans), bf16),
            in_specs=[pl.BlockSpec(memory_space=pltpu.HBM)] * 11,
            out_specs=pl.BlockSpec(memory_space=pltpu.VMEM),
            scratch_shapes=[
                vmem((per_dev * total, chans), bf16),
                vmem((per_dev * total, chans), bf16),
                vmem((total, 2 * half), bf16),
                vmem((total, half), bf16),
                vmem((row_tile, half), bf16),
                vmem((1, chans), f32), vmem((1, chans), f32),
                vmem((chans, 2 * half), bf16), vmem((1, 2 * half), f32),
                vmem((half,), f32), vmem((half,), f32),
                vmem((total, total), bf16), vmem((total, total), bf16),
                vmem((1, total), f32), vmem((total, 128), f32),
                vmem((half, chans), bf16), vmem((1, chans), f32),
                pltpu.SemaphoreType.REGULAR, pltpu.SemaphoreType.REGULAR,
                dma((10,)), dma((1,)), dma((per_dev,)), dma((1,)), dma((1,)),
            ],
            compiler_params=pltpu.CompilerParams(
                collective_id=0, has_side_effects=True, vmem_limit_bytes=56 * 1024 * 1024),
            name="gmlp",
        )(patches.reshape(n, per_dev, rows, chans), ln1_gain[None], ln1_bias[None], w_in, b_in[None],
          ln2_gain, ln2_bias, w_spatial, b_spatial[None], w_out, b_out[None])
        return out.reshape(images, rows, chans)

    return jax.shard_map(per_device, mesh=mesh, in_specs=in_specs, out_specs=row_spec, check_vma=False)
```

```python
import functools

import jax
import jax.numpy as jnp
from jax import lax
from jax.experimental import pallas as pl
from jax.experimental.pallas import tpu as pltpu
from jax.sharding import PartitionSpec as P

LN_EPS = 1e-6
MESH = pl.DeviceIdType.MESH
SQRT_HALF = 0.7071067811865476
GREET_STEPS = (4, 2, -2, 3, -3, 1, -1, 0)
IN_STEPS = (-2, 0, -1, 3, 2, 1, 4, -3)
OUT_STEPS = (4, 3, -3, -1, -2, 1, 0, 2)


def normalize(values_f, gain_vec, offset):
    mean_val = jnp.mean(values_f, axis=-1, keepdims=True)
    centered = values_f - mean_val
    var_val = jnp.mean(centered * centered, axis=-1, keepdims=True)
    return (centered * lax.rsqrt(var_val + LN_EPS) * gain_vec + offset).astype(jnp.bfloat16)


def kernel(n, row_tile, col_tile, x_hbm, g1_hbm, b1_hbm, wi_hbm, bi_hbm, g2_hbm, b2_hbm, ws_hbm, bs_hbm, wo_hbm, bo_hbm,
           out_ref, gath, ybuf, hbuf, nbuf, gbuf, g1, b1, wi, bi, g2, b2, ws, wst, bs, bst, wo, bo,
           answered, complete, w_sem, in_send, in_recv, out_send, out_recv):
    me = lax.axis_index("seq")
    per_dev, rows, chans = x_hbm.shape[1], x_hbm.shape[2], x_hbm.shape[3]
    patches = n * rows
    half = wo.shape[0]
    bf16, f32 = jnp.bfloat16, jnp.float32

    chips = n // 2
    chip, core = lax.div(me, 2), lax.rem(me, 2)

    def ring(steps):
        found = []
        for step in steps:
            there = 2 * lax.rem(chip + step + chips, chips)
            found += [there + core, there + 1 - core] if step else [there + 1 - core]
        assert len(found) == n - 1
        return found

    def by_index():
        return [i + (me <= i).astype(jnp.int32) for i in range(n - 1)]

    loads = [pltpu.make_async_copy(src, dst, w_sem.at[i]) for i, (src, dst) in enumerate((
        (g1_hbm, g1), (b1_hbm, b1), (wi_hbm, wi), (bi_hbm, bi), (g2_hbm, g2), (b2_hbm, b2),
        (ws_hbm, ws), (bs_hbm, bs), (wo_hbm, wo), (bo_hbm, bo)))]

    def mine(base):
        return pl.ds(pl.multiple_of(base * patches + me * rows, rows), rows)

    def send_in(j, to):
        pltpu.make_async_remote_copy(
            src_ref=x_hbm.at[to, j], dst_ref=gath.at[mine(j)], send_sem=in_send.at[0], recv_sem=in_recv.at[j],
            device_id={"seq": to}, device_id_type=MESH).start()

    barrier = pltpu.get_barrier_semaphore()
    span = n // 2
    low = me < span
    early = 2

    def tell(sem, to):
        pl.semaphore_signal(sem, inc=1, device_id={"seq": to}, device_id_type=MESH)

    def send_early(first):
        for j in range(early):
            for to in range(first, first + span):
                @pl.when(me != to)
                def _():
                    send_in(j, to)

    @pl.when(low)
    def _():
        for to in ring(GREET_STEPS):
            tell(barrier, to)

    for load in loads:
        load.start()
    pl.semaphore_wait(barrier, span - low.astype(jnp.int32))

    @pl.when(jnp.logical_not(low))
    def _():
        for to in range(span - 1, -1, -1):
            tell(answered, to)

    send_early(0)

    @pl.when(low)
    def _():
        pl.semaphore_wait(answered, span)
        tell(complete, n - 1 - me)

    @pl.when(jnp.logical_not(low))
    def _():
        pl.semaphore_wait(complete, 1)

    send_early(span)

    def send_late(j, carry):
        for to in ring(IN_STEPS):
            send_in(j, to)
        return carry

    lax.fori_loop(early, per_dev, send_late, 0)
    for j in range(per_dev):
        pltpu.make_async_copy(x_hbm.at[me, j], gath.at[mine(j)], in_recv.at[j]).start()

    for load in loads:
        load.wait()
    wst[...] = jnp.transpose(ws[...].astype(f32)).astype(bf16)
    bst[...] = jnp.transpose(jnp.broadcast_to(bs[...], (128, patches)))

    def one_image(j, carry):
        base = pl.multiple_of(j * patches, patches)
        image = gath.at[pl.ds(base, patches)]
        pltpu.make_async_copy(image, image, in_recv.at[j]).wait()

        def project(r, carry):
            start = pl.multiple_of(r * row_tile, row_tile)
            sl = pl.ds(start, row_tile)
            u = normalize(gath[pl.ds(pl.multiple_of(base + start, row_tile), row_tile), :].astype(f32), g1[...], b1[...])

            def column(c, carry):
                cs = pl.ds(pl.multiple_of(c * col_tile, col_tile), col_tile)
                hidden = jnp.dot(u, wi[:, cs], preferred_element_type=f32) + bi[:, cs]
                hbuf[sl, cs] = (0.5 * hidden * (1.0 + lax.erf(hidden * SQRT_HALF))).astype(bf16)
                return carry

            lax.fori_loop(0, 2 * half // col_tile, column, 0)

            def norm2(q, carry):
                qs = pl.ds(pl.multiple_of(start + q * 32, 32), 32)
                nbuf[qs, :] = normalize(hbuf[qs, half:].astype(f32), g2[...].reshape(1, half), b2[...].reshape(1, half))
                return carry

            lax.fori_loop(0, row_tile // 32, norm2, 0)
            return carry

        lax.fori_loop(0, patches // row_tile, project, 0)

        def mix(r, carry):
            start = pl.multiple_of(r * row_tile, row_tile)
            sl = pl.ds(start, row_tile)
            ysl = pl.ds(pl.multiple_of(base + start, row_tile), row_tile)
            bias = jnp.concatenate([bst[sl, :]] * (col_tile // 128), axis=1)

            def column(c, carry):
                cs = pl.ds(pl.multiple_of(c * col_tile, col_tile), col_tile)
                s = jnp.dot(wst[sl, :], nbuf[:, cs], preferred_element_type=f32).astype(bf16).astype(f32)
                gbuf[:, cs] = (hbuf[sl, cs].astype(f32) * (s + bias)).astype(bf16)
                return carry

            lax.fori_loop(0, half // col_tile, column, 0)
            mixed = jnp.dot(gbuf[...], wo[...], preferred_element_type=f32) + bo[...]
            ybuf[ysl, :] = (gath[ysl, :].astype(f32) + mixed).astype(bf16)
            return carry

        lax.fori_loop(0, patches // row_tile, mix, 0)

        def rows_of(dev):
            return pl.ds(pl.multiple_of(base + dev * rows, rows), rows)

        def send_out(to):
            pltpu.make_async_remote_copy(
                src_ref=ybuf.at[rows_of(to)], dst_ref=out_ref.at[me, j], send_sem=out_send.at[0], recv_sem=out_recv.at[0],
                device_id={"seq": to}, device_id_type=MESH).start()

        last = j == per_dev - 1
        for far, low in zip(ring(OUT_STEPS), by_index()):
            send_out(jnp.where(last, low, far))
        pltpu.make_async_copy(ybuf.at[rows_of(me)], out_ref.at[me, j], out_recv.at[0]).start()
        return carry

    lax.fori_loop(0, per_dev, one_image, 0)

    sent = pl.ds(0, per_dev * (n - 1) * rows)
    pltpu.make_async_copy(ybuf.at[sent], ybuf.at[sent], in_send.at[0]).wait()
    pltpu.make_async_copy(ybuf.at[sent], ybuf.at[sent], out_send.at[0]).wait()
    pltpu.make_async_copy(out_ref, out_ref, out_recv.at[0]).wait()


def solution(mesh):
    row_spec = P("data", "seq", None)
    vec_spec = P(None)
    mat_spec = P(None, None)
    in_specs = (row_spec, vec_spec, vec_spec, mat_spec, vec_spec, vec_spec, vec_spec, mat_spec, vec_spec, mat_spec, vec_spec)
    n = mesh.shape["seq"]

    def per_device(patches, ln1_gain, ln1_bias, w_in, b_in, ln2_gain, ln2_bias, w_spatial, b_spatial, w_out, b_out):
        images, rows, chans = patches.shape
        half = w_out.shape[0]
        per_dev = images // n
        total = n * rows
        row_tile, col_tile = 256, 512
        bf16, f32 = jnp.bfloat16, jnp.float32
        dma, vmem = pltpu.SemaphoreType.DMA, pltpu.VMEM
        out = pl.pallas_call(
            functools.partial(kernel, n, row_tile, col_tile),
            out_shape=pltpu.VMEM((n, per_dev, rows, chans), bf16),
            in_specs=[pl.BlockSpec(memory_space=pltpu.HBM)] * 11,
            out_specs=pl.BlockSpec(memory_space=pltpu.VMEM),
            scratch_shapes=[
                vmem((per_dev * total, chans), bf16),
                vmem((per_dev * total, chans), bf16),
                vmem((total, 2 * half), bf16),
                vmem((total, half), bf16),
                vmem((row_tile, half), bf16),
                vmem((1, chans), f32), vmem((1, chans), f32),
                vmem((chans, 2 * half), bf16), vmem((1, 2 * half), f32),
                vmem((half,), f32), vmem((half,), f32),
                vmem((total, total), bf16), vmem((total, total), bf16),
                vmem((1, total), f32), vmem((total, 128), f32),
                vmem((half, chans), bf16), vmem((1, chans), f32),
                pltpu.SemaphoreType.REGULAR, pltpu.SemaphoreType.REGULAR,
                dma((10,)), dma((1,)), dma((per_dev,)), dma((1,)), dma((1,)),
            ],
            compiler_params=pltpu.CompilerParams(
                collective_id=0, has_side_effects=True, vmem_limit_bytes=56 * 1024 * 1024),
            name="gmlp",
        )(patches.reshape(n, per_dev, rows, chans), ln1_gain[None], ln1_bias[None], w_in, b_in[None],
          ln2_gain, ln2_bias, w_spatial, b_spatial[None], w_out, b_out[None])
        return out.reshape(images, rows, chans)

    return jax.shard_map(per_device, mesh=mesh, in_specs=in_specs, out_specs=row_spec, check_vma=False)
```

```python
import functools

import jax
import jax.numpy as jnp
from jax import lax
from jax.experimental import pallas as pl
from jax.experimental.pallas import tpu as pltpu
from jax.sharding import PartitionSpec as P

LN_EPS = 1e-6
MESH = pl.DeviceIdType.MESH
SQRT_HALF = 0.7071067811865476
GREET_STEPS = (4, 2, -2, 3, -3, 1, -1, 0)
IN_STEPS = (-2, 0, -1, 3, 2, 1, 4, -3)
OUT_STEPS = (4, 3, -3, -1, -2, 1, 0, 2)


def normalize(values_f, gain_vec, offset):
    mean_val = jnp.mean(values_f, axis=-1, keepdims=True)
    centered = values_f - mean_val
    var_val = jnp.mean(centered * centered, axis=-1, keepdims=True)
    return (centered * lax.rsqrt(var_val + LN_EPS) * gain_vec + offset).astype(jnp.bfloat16)


def kernel(n, row_tile, col_tile, x_hbm, g1_hbm, b1_hbm, wi_hbm, bi_hbm, g2_hbm, b2_hbm, ws_hbm, bs_hbm, wo_hbm, bo_hbm,
           out_ref, gath, ybuf, hbuf, nbuf, gbuf, g1, b1, wi, bi, g2, b2, ws, wst, bs, bst, wo, bo,
           answered, complete, w_sem, in_send, in_recv, out_send, out_recv):
    me = lax.axis_index("seq")
    per_dev, rows, chans = x_hbm.shape[1], x_hbm.shape[2], x_hbm.shape[3]
    patches = n * rows
    half = wo.shape[0]
    bf16, f32 = jnp.bfloat16, jnp.float32

    chips = n // 2
    chip, core = lax.div(me, 2), lax.rem(me, 2)

    def ring(steps):
        found = []
        for step in steps:
            there = 2 * lax.rem(chip + step + chips, chips)
            found += [there + core, there + 1 - core] if step else [there + 1 - core]
        assert len(found) == n - 1
        return found

    def by_index():
        return [i + (me <= i).astype(jnp.int32) for i in range(n - 1)]

    loads = [pltpu.make_async_copy(src, dst, w_sem.at[i]) for i, (src, dst) in enumerate((
        (g1_hbm, g1), (b1_hbm, b1), (wi_hbm, wi), (bi_hbm, bi), (g2_hbm, g2), (b2_hbm, b2),
        (ws_hbm, ws), (bs_hbm, bs), (wo_hbm, wo), (bo_hbm, bo)))]

    def mine(base):
        return pl.ds(pl.multiple_of(base * patches + me * rows, rows), rows)

    def send_in(j, to):
        pltpu.make_async_remote_copy(
            src_ref=x_hbm.at[to, j], dst_ref=gath.at[mine(j)], send_sem=in_send.at[0], recv_sem=in_recv.at[j],
            device_id={"seq": to}, device_id_type=MESH).start()

    barrier = pltpu.get_barrier_semaphore()
    span = n // 2
    low = me < span
    early = 2

    def tell(sem, to):
        pl.semaphore_signal(sem, inc=1, device_id={"seq": to}, device_id_type=MESH)

    def send_early(first):
        for j in range(early):
            for to in range(first, first + span):
                @pl.when(me != to)
                def _():
                    send_in(j, to)

    @pl.when(low)
    def _():
        for to in ring(GREET_STEPS):
            tell(barrier, to)

    pl.semaphore_wait(barrier, span - low.astype(jnp.int32))

    @pl.when(jnp.logical_not(low))
    def _():
        for to in range(span - 1, -1, -1):
            tell(answered, to)

    send_early(0)
    for load in loads:
        load.start()

    @pl.when(low)
    def _():
        pl.semaphore_wait(answered, span)
        tell(complete, n - 1 - me)

    @pl.when(jnp.logical_not(low))
    def _():
        pl.semaphore_wait(complete, 1)

    send_early(span)

    def send_late(j, carry):
        for to in ring(IN_STEPS):
            send_in(j, to)
        return carry

    lax.fori_loop(early, per_dev, send_late, 0)
    for j in range(per_dev):
        pltpu.make_async_copy(x_hbm.at[me, j], gath.at[mine(j)], in_recv.at[j]).start()

    for load in loads:
        load.wait()
    wst[...] = jnp.transpose(ws[...].astype(f32)).astype(bf16)
    bst[...] = jnp.transpose(jnp.broadcast_to(bs[...], (128, patches)))

    def one_image(j, carry):
        base = pl.multiple_of(j * patches, patches)
        image = gath.at[pl.ds(base, patches)]
        pltpu.make_async_copy(image, image, in_recv.at[j]).wait()

        def project(r, carry):
            start = pl.multiple_of(r * row_tile, row_tile)
            sl = pl.ds(start, row_tile)
            u = normalize(gath[pl.ds(pl.multiple_of(base + start, row_tile), row_tile), :].astype(f32), g1[...], b1[...])

            def column(c, carry):
                cs = pl.ds(pl.multiple_of(c * col_tile, col_tile), col_tile)
                hidden = jnp.dot(u, wi[:, cs], preferred_element_type=f32) + bi[:, cs]
                hbuf[sl, cs] = (0.5 * hidden * (1.0 + lax.erf(hidden * SQRT_HALF))).astype(bf16)
                return carry

            lax.fori_loop(0, 2 * half // col_tile, column, 0)

            def norm2(q, carry):
                qs = pl.ds(pl.multiple_of(start + q * 32, 32), 32)
                nbuf[qs, :] = normalize(hbuf[qs, half:].astype(f32), g2[...].reshape(1, half), b2[...].reshape(1, half))
                return carry

            lax.fori_loop(0, row_tile // 32, norm2, 0)
            return carry

        lax.fori_loop(0, patches // row_tile, project, 0)

        def mix(r, carry):
            start = pl.multiple_of(r * row_tile, row_tile)
            sl = pl.ds(start, row_tile)
            ysl = pl.ds(pl.multiple_of(base + start, row_tile), row_tile)
            bias = jnp.concatenate([bst[sl, :]] * (col_tile // 128), axis=1)

            def column(c, carry):
                cs = pl.ds(pl.multiple_of(c * col_tile, col_tile), col_tile)
                s = jnp.dot(wst[sl, :], nbuf[:, cs], preferred_element_type=f32).astype(bf16).astype(f32)
                gbuf[:, cs] = (hbuf[sl, cs].astype(f32) * (s + bias)).astype(bf16)
                return carry

            lax.fori_loop(0, half // col_tile, column, 0)
            mixed = jnp.dot(gbuf[...], wo[...], preferred_element_type=f32) + bo[...]
            ybuf[ysl, :] = (gath[ysl, :].astype(f32) + mixed).astype(bf16)
            return carry

        lax.fori_loop(0, patches // row_tile, mix, 0)

        def rows_of(dev):
            return pl.ds(pl.multiple_of(base + dev * rows, rows), rows)

        def send_out(to):
            pltpu.make_async_remote_copy(
                src_ref=ybuf.at[rows_of(to)], dst_ref=out_ref.at[me, j], send_sem=out_send.at[0], recv_sem=out_recv.at[0],
                device_id={"seq": to}, device_id_type=MESH).start()

        last = j == per_dev - 1
        for far, low in zip(ring(OUT_STEPS), by_index()):
            send_out(jnp.where(last, low, far))
        pltpu.make_async_copy(ybuf.at[rows_of(me)], out_ref.at[me, j], out_recv.at[0]).start()
        return carry

    lax.fori_loop(0, per_dev, one_image, 0)

    sent = pl.ds(0, per_dev * (n - 1) * rows)
    pltpu.make_async_copy(ybuf.at[sent], ybuf.at[sent], in_send.at[0]).wait()
    pltpu.make_async_copy(ybuf.at[sent], ybuf.at[sent], out_send.at[0]).wait()
    pltpu.make_async_copy(out_ref, out_ref, out_recv.at[0]).wait()


def solution(mesh):
    row_spec = P("data", "seq", None)
    vec_spec = P(None)
    mat_spec = P(None, None)
    in_specs = (row_spec, vec_spec, vec_spec, mat_spec, vec_spec, vec_spec, vec_spec, mat_spec, vec_spec, mat_spec, vec_spec)
    n = mesh.shape["seq"]

    def per_device(patches, ln1_gain, ln1_bias, w_in, b_in, ln2_gain, ln2_bias, w_spatial, b_spatial, w_out, b_out):
        images, rows, chans = patches.shape
        half = w_out.shape[0]
        per_dev = images // n
        total = n * rows
        row_tile, col_tile = 256, 512
        bf16, f32 = jnp.bfloat16, jnp.float32
        dma, vmem = pltpu.SemaphoreType.DMA, pltpu.VMEM
        out = pl.pallas_call(
            functools.partial(kernel, n, row_tile, col_tile),
            out_shape=pltpu.VMEM((n, per_dev, rows, chans), bf16),
            in_specs=[pl.BlockSpec(memory_space=pltpu.HBM)] * 11,
            out_specs=pl.BlockSpec(memory_space=pltpu.VMEM),
            scratch_shapes=[
                vmem((per_dev * total, chans), bf16),
                vmem((per_dev * total, chans), bf16),
                vmem((total, 2 * half), bf16),
                vmem((total, half), bf16),
                vmem((row_tile, half), bf16),
                vmem((1, chans), f32), vmem((1, chans), f32),
                vmem((chans, 2 * half), bf16), vmem((1, 2 * half), f32),
                vmem((half,), f32), vmem((half,), f32),
                vmem((total, total), bf16), vmem((total, total), bf16),
                vmem((1, total), f32), vmem((total, 128), f32),
                vmem((half, chans), bf16), vmem((1, chans), f32),
                pltpu.SemaphoreType.REGULAR, pltpu.SemaphoreType.REGULAR,
                dma((10,)), dma((1,)), dma((per_dev,)), dma((1,)), dma((1,)),
            ],
            compiler_params=pltpu.CompilerParams(
                collective_id=0, has_side_effects=True, vmem_limit_bytes=56 * 1024 * 1024),
            name="gmlp",
        )(patches.reshape(n, per_dev, rows, chans), ln1_gain[None], ln1_bias[None], w_in, b_in[None],
          ln2_gain, ln2_bias, w_spatial, b_spatial[None], w_out, b_out[None])
        return out.reshape(images, rows, chans)

    return jax.shard_map(per_device, mesh=mesh, in_specs=in_specs, out_specs=row_spec, check_vma=False)
```
